32 devices in a mesh: band: 8 (over z, core), lane: 4 (over y, x).
Axes of the slice: x: 2, y: 2, z: 4, core: 2. Of those that a mesh axis runs over, the one named last changes fastest.
Arguments:
- first_factor: bfloat16 [8192, 4096], P('band', 'lane'), may hold values from -6 to 6
- second_factor: bfloat16 [4096, 2048], P('band', 'lane'), may hold values from -0.09375 to 0.09375
- result_in: float32 [8192, 2048], P('band', 'lane'), may hold values from -6 to 6
- pivot_scale: float32 [4096], replicated, may hold values from 0.25 to 1.75
Outputs:
- updated: float32 [8192, 2048], P('band', 'lane')
The draws below stay inside these ranges and needn't reach their ends.
All inputs are finite; a program needn't handle non-finite values.
Results may differ from the reference program's by a relative error of at most 0.002.
Values may be sent and summed in bfloat16 or wider, within the bound.
A program may use at most 128 MiB of HBM per device.

```python
import jax
import jax.numpy as jnp
from jax import lax

ROWS = 8192
COLS = 2048
INNER = 4096


def level_of(own_key, shape, split, least, top_value):
    factor_of = 1.0
    for axis_at, parts in split:
        steps = jax.random.uniform(jax.random.fold_in(jax.random.fold_in(own_key, 6), axis_at), (parts,), jnp.float32, least / len(split), top_value / len(split))
        factor_of = factor_of * jnp.repeat(jnp.exp(steps), shape[axis_at] // parts).reshape((-1,) + (1,) * (len(shape) - 1 - axis_at))
    return factor_of


def centred(own_key, shape, deviation, bound, split=(), held_as=jnp.bfloat16):
    result = jax.random.normal(own_key, shape, jnp.float32) * deviation
    if len(split) > 0:
        result = level_of(own_key, shape, split, -0.22, 0.18) * result
    return jnp.clip(result, min=-bound, max=bound).astype(held_as)


def setup_inputs(seed: int = 0) -> dict:
    key_list = jax.random.split(jax.random.key(seed), 5)
    first_factor = centred(key_list[0], (ROWS, INNER), 1.0, 6.0, ((0, 8), (1, 4)))
    second_factor = centred(key_list[1], (INNER, COLS), INNER ** -0.5, 0.09375, ((0, 8), (1, 4)))
    result_in = centred(key_list[2], (ROWS, COLS), 1.0, 6.0, ((0, 8), (1, 4)), jnp.float32)
    pivot_scale = jnp.clip(1.0 + 0.15 * jax.random.normal(key_list[3], (INNER,), jnp.float32), 0.25, 1.75)
    return {"first_factor": first_factor, "second_factor": second_factor, "result_in": result_in, "pivot_scale": pivot_scale}


def reference(first_factor, second_factor, result_in, pivot_scale):
    scaled_left = (first_factor.astype(jnp.float32) * pivot_scale).astype(jnp.bfloat16)
    updated = result_in - jnp.dot(scaled_left, second_factor, preferred_element_type=jnp.float32)
    row_power = lax.optimization_barrier(jnp.sum(updated * updated, axis=1))
    updated = updated * lax.rsqrt(row_power / COLS + 1e-06)[:, None]
    return updated
```

```python
import functools

import jax
import jax.numpy as jnp
from jax import lax
from jax.experimental import pallas as pl
from jax.experimental.pallas import tpu as pltpu
from jax.sharding import PartitionSpec as P

MESH = pl.DeviceIdType.MESH
PIECES = 4
CHUNKS = 8
X0, X1, D0, D1 = 0, 1, 2, 3

FIRST = (
    (("-D", 0, "u"),),
    (("-D", 0, "ud"), ("-D", 1, "u")),
    (("-D", 0, "y"), ("-D", 1, "y"), ("-D", 2, "y"), ("-D", 3, "y")),
    (
        ("-D", 0, "dy"), ("-D", 1, "dy"), ("-D", 2, "dy"), ("-D", 3, "dy"),
    ),
)
STEPS = (
    (
        ((D0, 0, ""), (D0, 1, ""), (D0, 2, ""), (D0, 3, ""), (X0, 0, "u")),
        ((D1, 0, ""), (D1, 1, ""), (D1, 2, ""), (D1, 3, ""), (X1, 0, "ud")),
        (("H", 0, "d"), (D1, 0, "u"), (D1, 1, "u")),
        (),
    ),
    (
        ((X0, 1, "u"), (X1, 0, ""), (X0, 2, "u"), (X1, 1, "")),
        ((X1, 1, "ud"), ("H", 0, "dy"), (X1, 2, "u"), ("H", 1, "dy")),
        (("H", 1, "d"), (X1, 0, "u"), ("H", 2, "d")),
        ((D1, 0, ""), (D1, 1, "")),
    ),
    (
        ((X0, 3, "u"), ("-D", 1, "u"), ("-D", 2, "u"), ("-D", 3, "u"), ("H", 0, "y"), ("H", 1, "y")),
        (
            (X1, 3, "u"), ("-D", 2, "u"), ("-D", 3, "u"), ("H", 2, "dy"), ("H", 3, "dy"),
            ("-X1", 2, "d"), ("-X1", 3, "d"), ("-D", 1, "d"), ("-D", 2, "d"), ("-D", 3, "d"),
        ),
        ((X1, 1, "u"), ("H", 3, "d"), (X0, 0, ""), (X1, 2, "u"), (X0, 1, "")),
        ((X1, 0, ""), (X1, 1, "")),
    ),
    (
        (("H", 2, "y"), ("H", 3, "y"), (X1, 2, ""), (X1, 3, "")),
        ((X0, 0, ""), (X0, 1, ""), (X0, 2, ""), (X0, 3, ""), (D0, 0, "u"), (D0, 1, "u")),
        ((X1, 3, "u"), (X0, 2, ""), (X0, 3, ""), (D1, 2, "u")),
        ((X1, 2, ""), (X1, 3, ""), (X0, 0, ""), (X0, 1, ""), (X0, 2, ""), (X0, 3, "")),
    ),
    (
        ((D1, 0, ""), (D1, 1, "")),
        ((D0, 2, "u"), (D0, 3, "u")),
        ((D1, 3, "u"),),
        ((D1, 2, ""),),
    ),
    (
        ((D1, 2, ""),),
        (),
        ((D0, 0, "u"), (D0, 1, "u")),
        ((D1, 3, ""), (D0, 0, "")),
    ),
    (
        ((D1, 3, ""),),
        (),
        ((D0, 2, "u"), (D0, 3, "u")),
        ((D0, 1, ""), (D0, 2, ""), (D0, 3, "")),
    ),
)


def gathered(first_factor, second_factor, result_in, pivot_scale):
    share = first_factor.shape[1]
    part_scale = lax.dynamic_slice_in_dim(pivot_scale, lax.axis_index("lane") * share, share)
    scaled_left = (first_factor.astype(jnp.float32) * part_scale).astype(jnp.bfloat16)
    left_line = lax.all_gather(scaled_left, "lane", axis=1, tiled=True)
    right = lax.all_gather(second_factor, "band", axis=0, tiled=True)
    updated = result_in - jnp.dot(left_line, right, preferred_element_type=jnp.float32)
    row_power = lax.psum(jnp.sum(updated * updated, axis=1), "lane")
    return (
        updated * lax.rsqrt(row_power / (updated.shape[1] * lax.axis_size("lane")) + 1e-06)[:, None]
    )


def kernel(
    chips, left_hbm, right_hbm, result_hbm, scale_ref, out_ref, power_ref,
    left, right, helper, result, outgoing, incoming, norm_out, norm_in,
    load_sem, left_send, left_recv, right_sem, helper_sem, up_sem, down_sem, across_sem,
    relay_sem, peer_send, peer_recv, part_send, part_recv, norm_send, norm_recv,
):
    band, lane = lax.axis_index("band"), lax.axis_index("lane")
    z, core = band // 2, band % 2
    y, x = lane // 2, lane % 2
    peer = (2 * z + 1 - core, lane)
    lane_x, lane_y, lane_d = 2 * y + 1 - x, 2 * (1 - y) + x, 2 * (1 - y) + 1 - x
    role = z * (1 - y) + (chips - 1 - z) * y
    above, below = (band + 2 - 4 * y, lane), (band - 2 + 4 * y, lane)
    across = (band, lane_y)
    rows, share = left_hbm.shape
    depth, width = right_hbm.shape
    piece = depth // PIECES
    chunk = rows // CHUNKS
    own_at = pl.multiple_of((x + y) % 2 * share, share)
    other_at = pl.multiple_of((x + y + 1) % 2 * share, share)

    def span(at):
        return pl.ds(pl.multiple_of(at * chunk, chunk), chunk)

    load_left = pltpu.make_async_copy(left_hbm, left.at[:, pl.ds(own_at, share)], load_sem.at[0])
    load_left.start()
    load_result = pltpu.make_async_copy(result_hbm, result, load_sem.at[1])

    barrier = pltpu.get_barrier_semaphore()
    for other in (lane_x, lane_y, lane_d):
        pl.semaphore_signal(barrier, inc=1, device_id=(band, other), device_id_type=MESH)
    pl.semaphore_signal(barrier, inc=1, device_id=peer, device_id_type=MESH)

    @pl.when(role < chips - 1)
    def _():
        pl.semaphore_signal(barrier, inc=1, device_id=above, device_id_type=MESH)

    @pl.when(role > 0)
    def _():
        pl.semaphore_signal(barrier, inc=1, device_id=below, device_id_type=MESH)

    pl.semaphore_wait(barrier, 4 + (role + chips - 1) // chips + (2 * chips - 2 - role) // chips)

    def left_copy(at):
        return pltpu.make_async_remote_copy(
            left_hbm.at[span(at), :], left.at[span(at), pl.ds(own_at, share)],
            left_send.at[at], left_recv.at[at], device_id=(band, lane_x), device_id_type=MESH,
        )

    def left_arrival(at):
        return pltpu.make_async_remote_copy(
            left_hbm.at[span(at), :], left.at[span(at), pl.ds(other_at, share)],
            left_send.at[at], left_recv.at[at], device_id=(band, lane_x), device_id_type=MESH,
        )

    def place(slot, part, of_core):
        start = pl.multiple_of((slot % 2 * 2 + of_core) * depth + part * piece, piece)
        return right.at[slot // 2, pl.ds(start, piece), :]

    def own_piece(part):
        return right_hbm.at[pl.ds(part * piece, piece), :]

    def send(of_role, item, part, way):
        if item == "-D":
            slot, source = (D0, D1, X1, X0)[of_role], own_piece(part)
        elif item == "H":
            slot, source = X0, helper.at[part]
        else:
            slot = X1 if item == "-X1" else item
            source = place(slot, part, core)
        at = slot * PIECES + part
        if way == "y":
            target, there, gone = place(slot, part, core), across, across_sem.at[part]
        elif way == "d" and (item == "H" or of_role == 3):
            target, there, gone = helper.at[part], below, relay_sem.at[part]
        elif way == "d":
            target, there, gone = place(slot, part, core), below, down_sem.at[at]
        else:
            target, there, gone = place(slot, part, core), above, up_sem.at[at]
        relayed = way == "d" and (item == "H" or of_role == 3)
        came = helper_sem.at[part] if relayed else right_sem.at[at]
        return pltpu.make_async_remote_copy(
            source, target, gone, came, device_id=there, device_id_type=MESH
        )

    def local_copy(slot, part):
        return pltpu.make_async_copy(
            own_piece(part), place(slot, part, core), right_sem.at[slot * PIECES + part]
        )

    def to_peer(slot, part, of_core):
        at = slot * PIECES + part
        ref = place(slot, part, of_core)
        return pltpu.make_async_remote_copy(
            ref, ref, peer_send.at[at], peer_recv.at[at], device_id=peer, device_id_type=MESH
        )

    def arrival(item, part):
        if item == "H":
            ref, came = helper.at[part], helper_sem.at[part]
        else:
            ref, came = place(item, part, core), right_sem.at[item * PIECES + part]
        return pltpu.make_async_remote_copy(
            ref, ref, came, came, device_id=peer, device_id_type=MESH
        )

    def take(of_role, steps):
        for item, part, ways in steps:
            if item in (X0, X1, D0, D1, "H"):
                arrival(item, part).wait_recv()
            for way in ways:
                send(of_role, item, part, way).start()
            if item in (X0, X1, D0, D1):
                to_peer(item, part, core).start()

    def by_role(table):
        for of_role in range(4):
            if table[of_role]:
                @pl.when(role == of_role)
                def _():
                    take(of_role, table[of_role])

    def await_peer(which):
        for slot in (2 * which, 2 * which + 1):
            for part in range(PIECES):
                to_peer(slot, part, 1 - core).wait_recv()

    def scale(at, start, of_lane):
        factor = scale_ref[:, pl.ds(pl.multiple_of(of_lane * share, share), share)]
        window = left.at[span(at), pl.ds(start, share)]
        window[...] = (window[...].astype(jnp.float32) * factor).astype(jnp.bfloat16)

    def take_left(at):
        left_arrival(at).wait_recv()
        scale(at, other_at, lane_x)

    def product(which, at):
        return jnp.dot(left[span(at), :], right[which], preferred_element_type=jnp.float32)

    def part_copy(at):
        return pltpu.make_async_remote_copy(
            outgoing.at[span(at), :], incoming.at[span(at), :], part_send.at[at],
            part_recv.at[at], device_id=across, device_id_type=MESH,
        )

    def send_part(at):
        outgoing[span(at), :] = product(0, at).astype(jnp.bfloat16)
        part_copy(at).start()

    def keep_part(at):
        out_ref[span(at), :] = result[span(at), :] - product(1, at)

    def finish(at):
        part_copy(at).wait_recv()
        updated = out_ref[span(at), :] - incoming[span(at), :].astype(jnp.float32)
        out_ref[span(at), :] = updated
        power = updated * updated
        power = sum(power[:, k : k + 128] for k in range(0, width, 128))
        norm_out[:, span(at)] = jnp.sum(power.T.reshape(16, 8, chunk), axis=0)

    last = CHUNKS - 1
    groups = (pl.ds(0, last * chunk), pl.ds(last * chunk, chunk))

    def norm_copy(group, k, other):
        return pltpu.make_async_remote_copy(
            norm_out.at[:, groups[group]], norm_in.at[k, :, groups[group]],
            norm_send.at[group, k], norm_recv.at[group, k],
            device_id=(band, other), device_id_type=MESH,
        )

    def norms(group):
        return [norm_copy(group, k, other) for k, other in enumerate((lane_x, lane_y, lane_d))]

    def total(group):
        for copy in norms(group):
            copy.wait_recv()
        at = groups[group]
        power = norm_out[:, at] + norm_in[0, :, at] + norm_in[1, :, at] + norm_in[2, :, at]
        power = jnp.sum(power, axis=0, keepdims=True)
        power_ref[at, :] = jnp.broadcast_to(power, (128, at.size)).T

    by_role(FIRST)
    for at in range(CHUNKS):
        left_copy(at).start()
    load_result.start()

    @pl.when(role == 0)
    def _():
        for part in range(PIECES):
            local_copy(D0, part).start()

    @pl.when(role == 1)
    def _():
        for part in range(PIECES):
            local_copy(D1, part).start()

    load_left.wait()
    pl.loop(0, CHUNKS)(lambda at: scale(at, own_at, lane))

    ready = 4
    for at in range(ready):
        by_role(STEPS[at])
        take_left(at)
    await_peer(0)
    pl.loop(0, ready)(send_part)
    for at in range(ready, last):
        by_role(STEPS[at])
        take_left(at)
        send_part(at)
    await_peer(1)
    load_result.wait()
    pl.loop(0, last)(keep_part)
    take_left(last)
    send_part(last)
    pl.loop(0, last)(finish)
    for copy in norms(0):
        copy.start()
    keep_part(last)
    finish(last)
    for copy in norms(1):
        copy.start()
    total(0)

    for at in range(CHUNKS):
        left_copy(at).wait_send()
        part_copy(at).wait_send()
    for of_role in range(4):
        @pl.when(role == of_role)
        def _():
            for table in (FIRST,) + STEPS:
                for item, part, ways in table[of_role]:
                    for way in ways:
                        send(of_role, item, part, way).wait_send()
    for slot in range(4):
        for part in range(PIECES):
            to_peer(slot, part, core).wait_send()
    total(1)
    for group in range(2):
        for copy in norms(group):
            copy.wait_send()


def on_device(chips, first_factor, second_factor, result_in, pivot_scale):
    rows, share = first_factor.shape
    depth, width = second_factor.shape
    slots = 4 * PIECES
    dma = pltpu.SemaphoreType.DMA
    flops = 2 * rows * share * 4 * width
    updated, power = pl.pallas_call(
        functools.partial(kernel, chips),
        out_shape=(
            jax.ShapeDtypeStruct((rows, width), jnp.float32),
            jax.ShapeDtypeStruct((rows, 128), jnp.float32),
        ),
        in_specs=[
            pl.BlockSpec(memory_space=pltpu.HBM),
            pl.BlockSpec(memory_space=pltpu.HBM),
            pl.BlockSpec(memory_space=pltpu.HBM),
            pl.BlockSpec(memory_space=pltpu.VMEM),
        ],
        out_specs=[pl.BlockSpec(memory_space=pltpu.VMEM)] * 2,
        scratch_shapes=[
            pltpu.VMEM((rows, 2 * share), jnp.bfloat16),
            pltpu.VMEM((2, 4 * depth, width), jnp.bfloat16),
            pltpu.VMEM((PIECES, depth // PIECES, width), jnp.bfloat16),
            pltpu.VMEM((rows, width), jnp.float32),
            pltpu.VMEM((rows, width), jnp.bfloat16),
            pltpu.VMEM((rows, width), jnp.bfloat16),
            pltpu.VMEM((8, rows), jnp.float32),
            pltpu.VMEM((3, 8, rows), jnp.float32),
            dma((2,)),
            dma((CHUNKS,)),
            dma((CHUNKS,)),
            dma((slots,)),
            dma((PIECES,)),
            dma((slots,)),
            dma((slots,)),
            dma((PIECES,)),
            dma((PIECES,)),
            dma((slots,)),
            dma((slots,)),
            dma((CHUNKS,)),
            dma((CHUNKS,)),
            dma((2, 3)),
            dma((2, 3)),
        ],
        compiler_params=pltpu.CompilerParams(
            collective_id=0, has_side_effects=True, vmem_limit_bytes=62 * 1024 * 1024
        ),
        cost_estimate=pl.CostEstimate(
            flops=flops, bytes_accessed=8 * rows * share, transcendentals=0
        ),
    )(first_factor, second_factor, result_in, pivot_scale.reshape(1, -1))
    return updated * lax.rsqrt(power[:, :1] / (width * lax.axis_size("lane")) + 1e-06)


def solution(mesh):
    bands, lanes = mesh.shape["band"], mesh.shape["lane"]

    def body(first_factor, second_factor, result_in, pivot_scale):
        fits = lanes == 4 and bands == 2 * lanes
        plan = functools.partial(on_device, bands // 2) if fits else gathered
        return plan(first_factor, second_factor, result_in, pivot_scale)

    return jax.shard_map(
        body,
        mesh=mesh,
        in_specs=(P("band", "lane"), P("band", "lane"), P("band", "lane"), P()),
        out_specs=P("band", "lane"),
        check_vma=False,
    )
```

```python
import functools
import heapq

import jax
import jax.numpy as jnp
from jax import lax
from jax.experimental import pallas as pl
from jax.experimental.pallas import tpu as pltpu
from jax.sharding import PartitionSpec as P

MESH = pl.DeviceIdType.MESH
PIECES = 8
CHUNKS = 8
TAIL = (64, 32, 32)
FIRST, SECOND = 2, 3
X0, X1, D0, D1, H = 0, 1, 2, 3, 4
START, BLOCK, HOP = 3.3, 11.6, 2.4


def route():
    half = PIECES // 2
    rank = {X0: 0, H: 0, X1: 1, D1: 4, D0: 5}

    def urgency(item, part):
        return rank[item] + (2 * (part // half) if item not in (D0, D1) else 0)

    here, queued, busy, order, events = {}, {}, {}, {}, []

    def push(when, kind, *what):
        heapq.heappush(events, (when, len(events), kind, what))

    def send(role, way, item, part, lands, when):
        link = (role, way)
        queued.setdefault(link, []).append((urgency(item, part), part, item, lands))
        push(when, "free", link)

    for part in range(PIECES):
        for role, item in ((0, D0), (1, D1), (3, H)):
            push(START, "land", role, item, part)
        send(2, "y", X1, part, (1, X1), START)
        send(3, "y", X0, part, (0, X0), START)
    while events:
        when, _, kind, what = heapq.heappop(events)
        if kind == "free":
            (link,) = what
            if busy.get(link, 0.0) > when + 1e-9 or not queued.get(link):
                continue
            queued[link].sort()
            _, part, item, (role, becomes) = queued[link].pop(0)
            order.setdefault(link, []).append((item, part))
            busy[link] = when + BLOCK / PIECES
            push(busy[link], "free", link)
            push(busy[link] + HOP, "land", role, becomes, part)
            continue
        role, item, part = what
        here[role, item, part] = when
        if item == H:
            if role > 1 or (role == 1 and part % half):
                send(role, "d", H, part, (role - 1, H), when)
            if role < 2:
                send(role, "y", H, part, (2 if role == 1 else 3, X0), when)
        elif role == 1 and item in (X1, D1):
            send(role, "d", item, part, (0, item), when)
        if (
            (item == D0 and role < 3)
            or (item in (X1, D1) and role in (1, 2))
            or (item == X0 and (role == 0 or (role == 2 and part % half == 0)))
        ):
            send(role, "u", item, part, (role + 1, item), when)
    plans = [[], [], [], []]
    for (role, item, part), when in here.items():
        if (role, item) != (3, H):
            plans[role].append((max(when, START + 1.0), -1, "wait", item, part))
    for (role, way), sends in order.items():
        issued = START
        for index, (item, part) in enumerate(sends):
            if role < 2 or way != "y":
                issued = max(issued, here[role, item, part])
            plans[role].append((issued, index, way, item, part))
    return [sorted(plan) for plan in plans]


def gathered(first_factor, second_factor, result_in, pivot_scale):
    share = first_factor.shape[1]
    part_scale = lax.dynamic_slice_in_dim(pivot_scale, lax.axis_index("lane") * share, share)
    scaled_left = (first_factor.astype(jnp.float32) * part_scale).astype(jnp.bfloat16)
    left_line = lax.all_gather(scaled_left, "lane", axis=1, tiled=True)
    right = lax.all_gather(second_factor, "band", axis=0, tiled=True)
    updated = result_in - jnp.dot(left_line, right, preferred_element_type=jnp.float32)
    row_power = lax.psum(jnp.sum(updated * updated, axis=1), "lane")
    return (
        updated * lax.rsqrt(row_power / (updated.shape[1] * lax.axis_size("lane")) + 1e-06)[:, None]
    )


def kernel(
    chips, left_hbm, right_hbm, result_hbm, scale_hbm, out_hbm,
    left, right, helper, result, factors, outgoing, incoming, norm_out, norm_in,
    load_sem, left_send, left_recv, right_sem, helper_sem, way_sem, peer_send, peer_recv,
    part_send, part_recv, norm_send, norm_recv, out_sem,
):
    band, lane = lax.axis_index("band"), lax.axis_index("lane")
    z, core = band // 2, band % 2
    y, x = lane // 2, lane % 2
    peer = (2 * z + 1 - core, lane)
    lane_x, lane_y, lane_d = 2 * y + 1 - x, 2 * (1 - y) + x, 2 * (1 - y) + 1 - x
    role = z * (1 - y) + (chips - 1 - z) * y
    above, below = (band + 2 - 4 * y, lane), (band - 2 + 4 * y, lane)
    across = (band, lane_y)
    rows, share = left_hbm.shape
    lanes = 4
    depth, width = right_hbm.shape
    half = PIECES // 2
    piece, wide = depth // half, width // 2
    chunk = rows // CHUNKS
    own_at = pl.multiple_of((x + y) % 2 * share, share)
    other_at = pl.multiple_of((x + y + 1) % 2 * share, share)

    last = CHUNKS - 1
    sizes = (chunk,) * last + TAIL
    begins = [sum(sizes[:at]) for at in range(len(sizes) + 1)]

    def span(at):
        if isinstance(at, int):
            return pl.ds(begins[at], sizes[at])
        return pl.ds(pl.multiple_of(at * chunk, chunk), chunk)

    load_left = pltpu.make_async_copy(left_hbm, left.at[:, pl.ds(own_at, share)], load_sem.at[0])
    load_left.start()
    load_factors = pltpu.make_async_copy(scale_hbm, factors, load_sem.at[2])
    load_factors.start()
    load_result = pltpu.make_async_copy(result_hbm, result, load_sem.at[1])

    barrier = pltpu.get_barrier_semaphore()
    for other in (lane_x, lane_y, lane_d):
        pl.semaphore_signal(barrier, inc=1, device_id=(band, other), device_id_type=MESH)
    pl.semaphore_signal(barrier, inc=1, device_id=peer, device_id_type=MESH)

    @pl.when(role < chips - 1)
    def _():
        pl.semaphore_signal(barrier, inc=1, device_id=above, device_id_type=MESH)

    @pl.when(role > 0)
    def _():
        pl.semaphore_signal(barrier, inc=1, device_id=below, device_id_type=MESH)

    pl.semaphore_wait(barrier, 4 + (role + chips - 1) // chips + (2 * chips - 2 - role) // chips)

    def left_copy(at):
        return pltpu.make_async_remote_copy(
            left_hbm.at[span(at), :], left.at[span(at), pl.ds(own_at, share)],
            left_send.at[0], left_recv.at[at], device_id=(band, lane_x), device_id_type=MESH,
        )

    def left_arrival(at):
        return pltpu.make_async_remote_copy(
            left_hbm.at[span(at), :], left.at[span(at), pl.ds(other_at, share)],
            left_send.at[0], left_recv.at[at], device_id=(band, lane_x), device_id_type=MESH,
        )

    def place(slot, part, of_core):
        start = (slot % 2 * 2 + of_core) * depth + part % half * piece
        return right.at[
            slot // 2 * 2 + part // half, pl.ds(pl.multiple_of(start, piece), piece), :
        ]

    def own_piece(part):
        return right_hbm.at[
            pl.ds(part % half * piece, piece), pl.ds(part // half * wide, wide)
        ]

    def send(of_role, way, item, part):
        slot = X0 if item == H else item
        at = slot * PIECES + part
        if slot == of_role + D0 or (of_role, way) == (2, "y") or of_role == 3:
            source = own_piece(part)
        else:
            source = helper.at[part] if item == H else place(slot, part, core)
        target, came = place(slot, part, core), right_sem.at[at]
        there, gone = {"u": above, "d": below, "y": across}[way], way_sem.at["udy".index(way)]
        if item == H and way == "d":
            target, came = helper.at[part], helper_sem.at[part]
        return pltpu.make_async_remote_copy(
            source, target, gone, came, device_id=there, device_id_type=MESH
        )

    def local_copy(slot, part):
        return pltpu.make_async_copy(
            own_piece(part), place(slot, part, core), right_sem.at[slot * PIECES + part]
        )

    def to_peer(slot, part, of_core):
        group = slot if slot // 2 else part // half
        ref = place(slot, part, of_core)
        return pltpu.make_async_remote_copy(
            ref, ref, peer_send.at[0], peer_recv.at[group], device_id=peer, device_id_type=MESH
        )

    def await_bytes(ref, semaphore):
        pltpu.make_async_copy(ref, ref, semaphore).wait()

    def await_pieces(count, semaphore):
        blocks = 4 if count % 4 == 0 else 2
        await_bytes(right.at[pl.ds(0, blocks), pl.ds(0, count // blocks * piece), :], semaphore)

    def arrival(item, part):
        if item == H:
            ref, came = helper.at[part], helper_sem.at[part]
        else:
            ref, came = place(item, part, core), right_sem.at[item * PIECES + part]
        return pltpu.make_async_remote_copy(
            ref, ref, came, came, device_id=peer, device_id_type=MESH
        )

    plans = route()

    reach = [
        [
            max(when for when, _, way, item, part in plan if way == "wait" and wanted(item, part))
            for wanted in (
                lambda item, part: item in (X0, X1) and part < half,
                lambda item, part: item in (X0, X1),
                lambda item, part: item == D1,
                lambda item, part: item in (D0, D1),
            )
        ]
        for plan in plans
    ]
    taken = [0.0] * 4

    def take(until, needs=((),) * 4):
        for of_role in range(4):
            due = max([until] + [reach[of_role][need] for need in needs[of_role]])
            steps = [step for step in plans[of_role] if taken[of_role] < step[0] <= due]
            taken[of_role] = due
            if not steps:
                continue

            @pl.when(role == of_role)
            def _():
                for _, _, way, item, part in steps:
                    if way != "wait":
                        send(of_role, way, item, part).start()
                        continue
                    arrival(item, part).wait_recv()
                    if item != H:
                        to_peer(item, part, core).start()

    def await_peer(group):
        await_pieces(PIECES, peer_recv.at[group])

    def scale(at, start, of_lane):
        factor = factors[:, pl.ds(pl.multiple_of(of_lane * share, share), share)]
        window = left.at[span(at), pl.ds(start, share)]
        window[...] = (window[...].astype(jnp.float32) * factor).astype(jnp.bfloat16)

    def take_left(at):
        left_arrival(at).wait_recv()
        scale(at, other_at, lane_x)

    def part_copy(side, at):
        return pltpu.make_async_remote_copy(
            outgoing.at[side, span(at), :], incoming.at[side, span(at), :],
            part_send.at[0], part_recv.at[(at >= last) * 1 if isinstance(at, int) else 0],
            device_id=across, device_id_type=MESH,
        )

    def send_part(side, at):
        part = jnp.dot(left[span(at), :], right[side], preferred_element_type=jnp.float32)
        outgoing[side, span(at), :] = part.astype(jnp.bfloat16)
        part_copy(side, at).start()

    def rows_of(at):
        return pl.ds(pl.multiple_of(at * chunk, chunk), chunk)

    def keep(block, at):
        inner = pl.ds(block * share, share)
        for side in range(2):
            columns = slice(side * wide, (side + 1) * wide)
            result[rows_of(at), columns] = result[rows_of(at), columns] - jnp.dot(
                left[rows_of(at), inner], right[2 + side, inner, :],
                preferred_element_type=jnp.float32,
            )

    def finish(at):
        power = jnp.zeros((chunk, 128), jnp.float32)
        for side in range(2):
            columns = slice(side * wide, (side + 1) * wide)
            updated = result[rows_of(at), columns] - incoming[side, rows_of(at), :].astype(
                jnp.float32
            )
            result[rows_of(at), columns] = updated
            for k in range(0, wide, 128):
                power += updated[:, k : k + 128] * updated[:, k : k + 128]
        norm_out[:, rows_of(at)] = jnp.sum(power.T.reshape(16, 8, chunk), axis=0)

    def norms(group):
        rows_at = pl.ds(group * last * chunk, chunk if group else last * chunk)
        return [
            pltpu.make_async_remote_copy(
                norm_out.at[:, rows_at], norm_in.at[k, :, rows_at],
                norm_send.at[0], norm_recv.at[group],
                device_id=(band, other), device_id_type=MESH,
            )
            for k, other in enumerate((lane_x, lane_y, lane_d))
        ]

    def out_copy(group):
        rows_at = pl.ds(group * last * chunk, chunk if group else last * chunk)
        return pltpu.make_async_copy(
            result.at[rows_at, :], out_hbm.at[rows_at, :], out_sem.at[group]
        )

    def rescale(at):
        power = norm_out[:, rows_of(at)]
        for k in range(3):
            power = power + norm_in[k, :, rows_of(at)]
        power = jnp.sum(power, axis=0, keepdims=True)
        factor = lax.rsqrt(power / (width * lanes) + 1e-06)
        factor = jnp.broadcast_to(factor, (128, chunk)).T
        for k in range(0, width, 128):
            result[rows_of(at), k : k + 128] = result[rows_of(at), k : k + 128] * factor

    scope = jax.named_scope
    for at in range(len(sizes)):
        left_copy(at).start()
    take(START)

    @pl.when(role == 0)
    def _():
        for part in range(PIECES):
            local_copy(D0, part).start()

    @pl.when(role == 1)
    def _():
        for part in range(PIECES):
            local_copy(D1, part).start()

    load_result.start()
    with scope("own"):
        load_factors.wait()
        load_left.wait()
        pl.loop(0, CHUNKS)(lambda at: scale(at, own_at, lane))

    def keep_most():
        with scope("await_d0"):
            await_peer(D0)
        with scope("keep_d0"):
            pl.loop(0, last - 1)(lambda i: keep(0, i))

    needed = {
        FIRST: ((0,),) * 4,
        SECOND: ((1,),) * 4,
        last - 2: ((2, 3), (2, 3), (2,), (2,)),
        last - 1: ((), (), (3,), ()),
        len(sizes) - 1: ((), (), (), (3,)),
    }
    for at in range(len(sizes)):
        due = START + 4 * BLOCK * begins[at + 1] / rows + 0.7
        with scope(f"take{at}"):
            take(due, needed.get(at, ((),) * 4))
        with scope(f"left{at}"):
            left_arrival(at).wait_recv()
        with scope(f"scale{at}"):
            scale(at, other_at, lane_x)
        for side, ready in ((0, FIRST), (1, SECOND)):
            if at == ready:
                with scope(f"await_x{side}"):
                    await_peer(side)
                with scope(f"parts{side}"):
                    pl.loop(0, ready + 1)(lambda i: send_part(side, i))
            elif at > ready:
                with scope(f"part{side}_{at}"):
                    send_part(side, at)
        if at == last - 2:
            with scope("await_d1"):
                await_peer(D1)
                load_result.wait()
            with scope("keep_d1"):
                pl.loop(0, last - 1)(lambda i: keep(1, i))
            pl.when(role < 2)(keep_most)
        if at == last - 1:
            pl.when(role == 2)(keep_most)
    pl.when(role == 3)(keep_most)
    with scope("keep_rest"):
        for at in range(last - 1, CHUNKS):
            keep(1, at)
            keep(0, at)
    with scope("await_parts"):
        await_bytes(incoming.at[:, pl.ds(0, last * chunk), :], part_recv.at[0])
    with scope("finish"):
        pl.loop(0, last)(finish)
        for copy in norms(0):
            copy.start()
    with scope("await_tail"):
        await_bytes(incoming.at[:, pl.ds(last * chunk, chunk), :], part_recv.at[1])
    with scope("finish_tail"):
        finish(last)
        for copy in norms(1):
            copy.start()
    with scope("await_norm0"):
        await_bytes(norm_in.at[:, :, pl.ds(0, last * chunk)], norm_recv.at[0])
    with scope("rescale0"):
        pl.loop(0, last)(rescale)
        out_copy(0).start()
    with scope("await_norm1"):
        await_bytes(norm_in.at[:, :, pl.ds(last * chunk, chunk)], norm_recv.at[1])
    with scope("rescale1"):
        rescale(last)
        out_copy(1).start()

    with scope("sends"):
        await_bytes(left_hbm, left_send.at[0])
        await_bytes(outgoing, part_send.at[0])
        await_bytes(norm_in, norm_send.at[0])
        await_pieces(4 * PIECES, peer_send.at[0])
        for of_role in range(4):
            @pl.when(role == of_role)
            def _():
                for index, way in enumerate("udy"):
                    count = sum(step[2] == way for step in plans[of_role])
                    if count:
                        await_pieces(count, way_sem.at[index])
    with scope("out"):
        for group in range(2):
            out_copy(group).wait()


def on_device(chips, first_factor, second_factor, result_in, pivot_scale):
    rows, share = first_factor.shape
    depth, width = second_factor.shape
    slots, parts = 4 * PIECES, CHUNKS - 1 + len(TAIL)
    dma = pltpu.SemaphoreType.DMA
    flops = 2 * rows * share * 4 * width
    return pl.pallas_call(
        functools.partial(kernel, chips),
        out_shape=pltpu.VMEM((rows, width), jnp.float32),
        in_specs=[
            pl.BlockSpec(memory_space=pltpu.HBM),
            pl.BlockSpec(memory_space=pltpu.HBM),
            pl.BlockSpec(memory_space=pltpu.HBM),
            pl.BlockSpec(memory_space=pltpu.HBM),
        ],
        out_specs=pl.BlockSpec(memory_space=pl.ANY),
        scratch_shapes=[
            pltpu.VMEM((rows, 2 * share), jnp.bfloat16),
            pltpu.VMEM((4, 4 * depth, width // 2), jnp.bfloat16),
            pltpu.VMEM((PIECES, 2 * depth // PIECES, width // 2), jnp.bfloat16),
            pltpu.VMEM((rows, width), jnp.float32),
            pltpu.VMEM((1, 4 * share), jnp.float32),
            pltpu.VMEM((2, rows, width // 2), jnp.bfloat16),
            pltpu.VMEM((2, rows, width // 2), jnp.bfloat16),
            pltpu.VMEM((8, rows), jnp.float32),
            pltpu.VMEM((3, 8, rows), jnp.float32),
            dma((3,)),
            dma((1,)),
            dma((parts,)),
            dma((slots,)),
            dma((PIECES,)),
            dma((3,)),
            dma((1,)),
            dma((4,)),
            dma((1,)),
            dma((2,)),
            dma((1,)),
            dma((2,)),
            dma((2,)),
        ],
        compiler_params=pltpu.CompilerParams(
            collective_id=0, has_side_effects=True, vmem_limit_bytes=56 * 1024 * 1024
        ),
        cost_estimate=pl.CostEstimate(
            flops=flops, bytes_accessed=8 * rows * share, transcendentals=0
        ),
    )(first_factor, second_factor, result_in, pivot_scale.reshape(1, -1))


def solution(mesh):
    bands, lanes = mesh.shape["band"], mesh.shape["lane"]

    def body(first_factor, second_factor, result_in, pivot_scale):
        fits = lanes == 4 and bands == 2 * lanes
        plan = functools.partial(on_device, bands // 2) if fits else gathered
        return plan(first_factor, second_factor, result_in, pivot_scale)

    return jax.shard_map(
        body,
        mesh=mesh,
        in_specs=(P("band", "lane"), P("band", "lane"), P("band", "lane"), P()),
        out_specs=P("band", "lane"),
        check_vma=False,
    )
```

```python
import functools
import heapq

import jax
import jax.numpy as jnp
from jax import lax
from jax.experimental import pallas as pl
from jax.experimental.pallas import tpu as pltpu
from jax.sharding import PartitionSpec as P

MESH = pl.DeviceIdType.MESH
PIECES = 8
CHUNKS = 8
RELAYED = (1, 2, 3, 6, 7)
TAIL = (64, 32, 32)
FIRST, SECOND = 2, 3
X0, X1, D0, D1, H = 0, 1, 2, 3, 4
START, BLOCK, HOP = 3.3, 11.6, 2.4


def route():
    half = PIECES // 2
    rank = {X0: 0, H: 0, X1: 1, D1: 4, D0: 5}

    def urgency(item, part):
        return rank[item] + (2 * (part // half) if item not in (D0, D1) else 0)

    here, queued, busy, order, events = {}, {}, {}, {}, []

    def push(when, kind, *what):
        heapq.heappush(events, (when, len(events), kind, what))

    def send(role, way, item, part, lands, when):
        link = (role, way)
        queued.setdefault(link, []).append((urgency(item, part), part, item, lands))
        push(when, "free", link)

    for part in range(PIECES):
        for role, item in ((0, D0), (1, D1), (3, H)):
            push(START, "land", role, item, part)
        send(2, "y", X1, part, (1, X1), START)
        send(3, "y", X0, part, (0, X0), START)
    while events:
        when, _, kind, what = heapq.heappop(events)
        if kind == "free":
            (link,) = what
            if busy.get(link, 0.0) > when + 1e-9 or not queued.get(link):
                continue
            queued[link].sort()
            _, part, item, (role, becomes) = queued[link].pop(0)
            order.setdefault(link, []).append((item, part))
            busy[link] = when + BLOCK / PIECES
            push(busy[link], "free", link)
            push(busy[link] + HOP, "land", role, becomes, part)
            continue
        role, item, part = what
        here[role, item, part] = when
        if item == H:
            if role > 1 or (role == 1 and part in RELAYED):
                send(role, "d", H, part, (role - 1, H), when)
            if role < 2:
                send(role, "y", H, part, (2 if role == 1 else 3, X0), when)
        elif role == 1 and item in (X1, D1):
            send(role, "d", item, part, (0, item), when)
        if (
            (item == D0 and role < 3)
            or (item in (X1, D1) and role in (1, 2))
            or (item == X0 and (role == 0 or (role == 2 and part not in RELAYED)))
        ):
            send(role, "u", item, part, (role + 1, item), when)
    plans = [[], [], [], []]
    for (role, item, part), when in here.items():
        if (role, item) != (3, H):
            plans[role].append((max(when, START + 1.0), -1, "wait", item, part))
    for (role, way), sends in order.items():
        issued = START
        for index, (item, part) in enumerate(sends):
            if role < 2 or way != "y":
                issued = max(issued, here[role, item, part])
            plans[role].append((issued, index, way, item, part))
    return [sorted(plan) for plan in plans]


def gathered(first_factor, second_factor, result_in, pivot_scale):
    share = first_factor.shape[1]
    part_scale = lax.dynamic_slice_in_dim(pivot_scale, lax.axis_index("lane") * share, share)
    scaled_left = (first_factor.astype(jnp.float32) * part_scale).astype(jnp.bfloat16)
    left_line = lax.all_gather(scaled_left, "lane", axis=1, tiled=True)
    right = lax.all_gather(second_factor, "band", axis=0, tiled=True)
    updated = result_in - jnp.dot(left_line, right, preferred_element_type=jnp.float32)
    row_power = lax.psum(jnp.sum(updated * updated, axis=1), "lane")
    return (
        updated * lax.rsqrt(row_power / (updated.shape[1] * lax.axis_size("lane")) + 1e-06)[:, None]
    )


def kernel(
    chips, left_hbm, right_hbm, result_hbm, scale_hbm, out_hbm,
    left, right, helper, result, factors, early, outgoing, incoming, norm_out, norm_in,
    load_sem, left_send, left_recv, right_sem, helper_sem, way_sem, peer_send, peer_recv,
    part_send, part_recv, norm_send, norm_recv, out_sem,
):
    band, lane = lax.axis_index("band"), lax.axis_index("lane")
    z, core = band // 2, band % 2
    y, x = lane // 2, lane % 2
    peer = (2 * z + 1 - core, lane)
    lane_x, lane_y, lane_d = 2 * y + 1 - x, 2 * (1 - y) + x, 2 * (1 - y) + 1 - x
    role = z * (1 - y) + (chips - 1 - z) * y
    above, below = (band + 2 - 4 * y, lane), (band - 2 + 4 * y, lane)
    across = (band, lane_y)
    rows, share = left_hbm.shape
    lanes = 4
    depth, width = right_hbm.shape
    half = PIECES // 2
    piece, wide = depth // half, width // 2
    chunk = rows // CHUNKS
    own_at = pl.multiple_of((x + y) % 2 * share, share)
    other_at = pl.multiple_of((x + y + 1) % 2 * share, share)

    last = CHUNKS - 1
    sizes = (chunk,) * last + TAIL
    begins = [sum(sizes[:at]) for at in range(len(sizes) + 1)]

    def span(at):
        if isinstance(at, int):
            return pl.ds(begins[at], sizes[at])
        return pl.ds(pl.multiple_of(at * chunk, chunk), chunk)

    load_left = pltpu.make_async_copy(left_hbm, left.at[:, pl.ds(own_at, share)], load_sem.at[0])
    load_left.start()
    load_factors = pltpu.make_async_copy(scale_hbm, factors, load_sem.at[2])
    load_factors.start()
    load_result = pltpu.make_async_copy(result_hbm, result, load_sem.at[1])

    barrier = pltpu.get_barrier_semaphore()
    for other in (lane_x, lane_y):
        pl.semaphore_signal(barrier, inc=1, device_id=(band, other), device_id_type=MESH)
    pl.semaphore_signal(barrier, inc=1, device_id=peer, device_id_type=MESH)

    @pl.when(role < chips - 1)
    def _():
        pl.semaphore_signal(barrier, inc=1, device_id=above, device_id_type=MESH)

    @pl.when(role > 0)
    def _():
        pl.semaphore_signal(barrier, inc=1, device_id=below, device_id_type=MESH)

    pl.semaphore_wait(barrier, 3 + (role + chips - 1) // chips + (2 * chips - 2 - role) // chips)

    def left_copy(at):
        return pltpu.make_async_remote_copy(
            left_hbm.at[span(at), :], left.at[span(at), pl.ds(own_at, share)],
            left_send.at[0], left_recv.at[at], device_id=(band, lane_x), device_id_type=MESH,
        )

    def left_arrival(at):
        return pltpu.make_async_remote_copy(
            left_hbm.at[span(at), :], left.at[span(at), pl.ds(other_at, share)],
            left_send.at[0], left_recv.at[at], device_id=(band, lane_x), device_id_type=MESH,
        )

    def place(slot, part, of_core):
        start = (slot % 2 * 2 + of_core) * depth + part % half * piece
        return right.at[
            slot // 2 * 2 + part // half, pl.ds(pl.multiple_of(start, piece), piece), :
        ]

    def own_piece(part):
        return right_hbm.at[
            pl.ds(part % half * piece, piece), pl.ds(part // half * wide, wide)
        ]

    def send(of_role, way, item, part):
        slot = X0 if item == H else item
        at = slot * PIECES + part
        if slot == of_role + D0 or (of_role, way) == (2, "y") or of_role == 3:
            source = own_piece(part)
        else:
            source = helper.at[part] if item == H else place(slot, part, core)
        target, came = place(slot, part, core), right_sem.at[at]
        there, gone = {"u": above, "d": below, "y": across}[way], way_sem.at["udy".index(way)]
        if item == H and way == "d":
            target, came = helper.at[part], helper_sem.at[part]
        return pltpu.make_async_remote_copy(
            source, target, gone, came, device_id=there, device_id_type=MESH
        )

    def local_copy(slot, part):
        return pltpu.make_async_copy(
            own_piece(part), place(slot, part, core), right_sem.at[slot * PIECES + part]
        )

    def to_peer(slot, part, of_core):
        group = {X0: 0, X1: 0, D1: 2, D0: 3}[slot] + (slot != D1) * (part // half)
        ref = place(slot, part, of_core)
        return pltpu.make_async_remote_copy(
            ref, ref, peer_send.at[0], peer_recv.at[group], device_id=peer, device_id_type=MESH
        )

    def await_bytes(ref, semaphore):
        pltpu.make_async_copy(ref, ref, semaphore).wait()

    def await_pieces(count, semaphore):
        blocks = next(k for k in (4, 3, 2, 1) if count % k == 0)
        await_bytes(right.at[pl.ds(0, blocks), pl.ds(0, count // blocks * piece), :], semaphore)

    def arrival(item, part):
        if item == H:
            ref, came = helper.at[part], helper_sem.at[part]
        else:
            ref, came = place(item, part, core), right_sem.at[item * PIECES + part]
        return pltpu.make_async_remote_copy(
            ref, ref, came, came, device_id=peer, device_id_type=MESH
        )

    plans = route()

    reach = [
        [
            max(when for when, _, way, item, part in plan if way == "wait" and wanted(item, part))
            for wanted in (
                lambda item, part: item in (X0, X1) and part < half,
                lambda item, part: item in (X0, X1),
                lambda item, part: item == D1,
                lambda item, part: item == D0 and part < half,
                lambda item, part: item in (D0, D1),
            )
        ]
        for plan in plans
    ]
    taken = [0.0] * 4

    def take(until, needs=((),) * 4):
        for of_role in range(4):
            due = max([until] + [reach[of_role][need] for need in needs[of_role]])
            steps = [step for step in plans[of_role] if taken[of_role] < step[0] <= due]
            taken[of_role] = max(due, taken[of_role])
            if not steps:
                continue

            @pl.when(role == of_role)
            def _():
                for _, _, way, item, part in steps:
                    if way != "wait":
                        send(of_role, way, item, part).start()
                        continue
                    arrival(item, part).wait_recv()
                    if item != H:
                        to_peer(item, part, core).start()

    def await_peer(group):
        await_pieces(PIECES if group < 3 else half, peer_recv.at[group])

    def scale(at, start, of_lane):
        factor = factors[:, pl.ds(pl.multiple_of(of_lane * share, share), share)]
        window = left.at[span(at), pl.ds(start, share)]
        window[...] = (window[...].astype(jnp.float32) * factor).astype(jnp.bfloat16)

    def take_left(at):
        left_arrival(at).wait_recv()
        scale(at, other_at, lane_x)

    def part_copy(side, at):
        return pltpu.make_async_remote_copy(
            outgoing.at[side, span(at), :], incoming.at[side, span(at), :],
            part_send.at[0], part_recv.at[(at >= last) * 1 if isinstance(at, int) else 0],
            device_id=across, device_id_type=MESH,
        )

    def partial(side, rows_at, inner):
        return jnp.dot(
            left[rows_at, inner], right[side, inner, :], preferred_element_type=jnp.float32
        )

    def send_part(side, at):
        if isinstance(at, int) and at >= last:
            early_at = pl.ds(begins[at] - last * chunk, sizes[at])
            part = early[side, early_at, :] + partial(side, span(at), pl.ds(other_at, share))
        else:
            part = partial(side, span(at), pl.ds(0, 2 * share))
        outgoing[side, span(at), :] = part.astype(jnp.bfloat16)
        part_copy(side, at).start()

    def rows_of(at):
        return pl.ds(pl.multiple_of(at * chunk, chunk), chunk)

    def keep(block, at, sides=(0, 1)):
        inner = pl.ds(block * share, share)
        for side in sides:
            columns = slice(side * wide, (side + 1) * wide)
            result[rows_of(at), columns] = result[rows_of(at), columns] - jnp.dot(
                left[rows_of(at), inner], right[2 + side, inner, :],
                preferred_element_type=jnp.float32,
            )

    def finish(at):
        power = jnp.zeros((chunk, 128), jnp.float32)
        for side in range(2):
            columns = slice(side * wide, (side + 1) * wide)
            updated = result[rows_of(at), columns] - incoming[side, rows_of(at), :].astype(
                jnp.float32
            )
            result[rows_of(at), columns] = updated
            for k in range(0, wide, 128):
                power += updated[:, k : k + 128] * updated[:, k : k + 128]
        norm_out[:, rows_of(at)] = jnp.sum(power.T, axis=0, keepdims=True)

    def norms(group):
        rows_at = pl.ds(group * last * chunk, chunk if group else last * chunk)
        return [
            pltpu.make_async_remote_copy(
                norm_out.at[:, rows_at], norm_in.at[k, :, rows_at],
                norm_send.at[0], norm_recv.at[group],
                device_id=(band, other), device_id_type=MESH,
            )
            for k, other in enumerate((lane_x, lane_y, lane_d))
        ]

    def out_copy(group):
        rows_at = pl.ds(group * last * chunk, chunk if group else last * chunk)
        return pltpu.make_async_copy(
            result.at[rows_at, :], out_hbm.at[rows_at, :], out_sem.at[group]
        )

    def rescale(at):
        power = norm_out[:, rows_of(at)]
        for k in range(3):
            power = power + norm_in[k, :, rows_of(at)]
        factor = lax.rsqrt(power / (width * lanes) + 1e-06)
        factor = jnp.broadcast_to(factor, (128, chunk)).T
        for k in range(0, width, 128):
            result[rows_of(at), k : k + 128] = result[rows_of(at), k : k + 128] * factor

    scope = jax.named_scope
    for at in range(len(sizes)):
        left_copy(at).start()
    take(START)

    @pl.when(role == 0)
    def _():
        for part in range(PIECES):
            local_copy(D0, part).start()

    @pl.when(role == 1)
    def _():
        for part in range(PIECES):
            local_copy(D1, part).start()

    load_result.start()
    with scope("own"):
        load_factors.wait()
        load_left.wait()
        pl.loop(0, CHUNKS)(lambda at: scale(at, own_at, lane))

    def keep_some(block, begin, end, sides=(0, 1)):
        with scope(f"keep{block}_{end}_{sides[0]}"):
            pl.loop(begin, end)(lambda i: keep(block, i, sides))

    needed = {
        last - 2: ((2, 4), (2, 4), (2,), (2,)),
        last - 1: ((), (), (4,), (3,)),
        len(sizes) - 1: ((), (), (), (4,)),
    }
    for at in range(len(sizes)):
        due = START + 4 * BLOCK * begins[at + 1] / rows + 0.7
        with scope(f"take{at}"):
            take(due, needed.get(at, ((),) * 4))
        with scope(f"left{at}"):
            left_arrival(at).wait_recv()
        with scope(f"scale{at}"):
            scale(at, other_at, lane_x)
        for side, ready in ((0, FIRST), (1, SECOND)):
            if at == ready:
                take(0.0, ((side,),) * 4)
                with scope(f"await_x{side}"):
                    await_peer(side)
                with scope(f"parts{side}"):
                    pl.loop(0, ready + 1)(lambda i: send_part(side, i))
            elif at > ready:
                with scope(f"part{side}_{at}"):
                    send_part(side, at)
        if at == SECOND:
            with scope("early"):
                for side in range(2):
                    early[side] = partial(
                        side, pl.ds(last * chunk, chunk), pl.ds(own_at, share)
                    )
        if at == last - 2:
            with scope("await_d1"):
                await_peer(2)
                load_result.wait()
            keep_some(1, 0, last - 1)

            @pl.when(role < 2)
            def _():
                await_peer(3)
                await_peer(4)
                keep_some(0, 0, last - 1)
        if at == last - 1:
            keep(1, last - 1)

            @pl.when(role < 2)
            def _():
                keep(0, last - 1)

            @pl.when(role == 2)
            def _():
                await_peer(3)
                await_peer(4)
                keep_some(0, 0, 3)

            @pl.when(role == 3)
            def _():
                await_peer(3)
                keep_some(0, 0, last - 1, (0,))

    @pl.when(role == 2)
    def _():
        keep_some(0, 3, last)

    @pl.when(role == 3)
    def _():
        keep(0, last - 1, (0,))
        await_peer(4)
        keep_some(0, 0, last, (1,))

    with scope("await_parts"):
        await_bytes(incoming.at[:, pl.ds(0, last * chunk), :], part_recv.at[0])
    with scope("finish"):
        pl.loop(0, last, unroll=True)(finish)
        for copy in norms(0):
            copy.start()
    with scope("keep_last"):
        keep(1, last)
        keep(0, last)
    with scope("await_tail"):
        await_bytes(incoming.at[:, pl.ds(last * chunk, chunk), :], part_recv.at[1])
    with scope("finish_tail"):
        finish(last)
        for copy in norms(1):
            copy.start()
    with scope("await_norm0"):
        await_bytes(norm_in.at[:, :, pl.ds(0, last * chunk)], norm_recv.at[0])
    with scope("rescale0"):
        pl.loop(0, last, unroll=True)(rescale)
        out_copy(0).start()
    with scope("await_norm1"):
        await_bytes(norm_in.at[:, :, pl.ds(last * chunk, chunk)], norm_recv.at[1])
    with scope("rescale1"):
        rescale(last)
        out_copy(1).start()

    with scope("sends"):
        await_bytes(left_hbm, left_send.at[0])
        await_bytes(outgoing, part_send.at[0])
        await_bytes(norm_in, norm_send.at[0])
        await_pieces(4 * PIECES, peer_send.at[0])
        for of_role in range(4):
            @pl.when(role == of_role)
            def _():
                for index, way in enumerate("udy"):
                    count = sum(step[2] == way for step in plans[of_role])
                    if count:
                        await_pieces(count, way_sem.at[index])
    with scope("out"):
        for group in range(2):
            out_copy(group).wait()


def on_device(chips, first_factor, second_factor, result_in, pivot_scale):
    rows, share = first_factor.shape
    depth, width = second_factor.shape
    slots, parts = 4 * PIECES, CHUNKS - 1 + len(TAIL)
    dma = pltpu.SemaphoreType.DMA
    flops = 2 * rows * share * 4 * width
    return pl.pallas_call(
        functools.partial(kernel, chips),
        out_shape=pltpu.VMEM((rows, width), jnp.float32),
        in_specs=[
            pl.BlockSpec(memory_space=pltpu.HBM),
            pl.BlockSpec(memory_space=pltpu.HBM),
            pl.BlockSpec(memory_space=pltpu.HBM),
            pl.BlockSpec(memory_space=pltpu.HBM),
        ],
        out_specs=pl.BlockSpec(memory_space=pl.ANY),
        scratch_shapes=[
            pltpu.VMEM((rows, 2 * share), jnp.bfloat16),
            pltpu.VMEM((4, 4 * depth, width // 2), jnp.bfloat16),
            pltpu.VMEM((PIECES, 2 * depth // PIECES, width // 2), jnp.bfloat16),
            pltpu.VMEM((rows, width), jnp.float32),
            pltpu.VMEM((1, 4 * share), jnp.float32),
            pltpu.VMEM((2, rows // CHUNKS, width // 2), jnp.float32),
            pltpu.VMEM((2, rows, width // 2), jnp.bfloat16),
            pltpu.VMEM((2, rows, width // 2), jnp.bfloat16),
            pltpu.VMEM((1, rows), jnp.float32),
            pltpu.VMEM((3, 1, rows), jnp.float32),
            dma((3,)),
            dma((1,)),
            dma((parts,)),
            dma((slots,)),
            dma((PIECES,)),
            dma((3,)),
            dma((1,)),
            dma((5,)),
            dma((1,)),
            dma((2,)),
            dma((1,)),
            dma((2,)),
            dma((2,)),
        ],
        compiler_params=pltpu.CompilerParams(
            collective_id=0, has_side_effects=True, vmem_limit_bytes=56 * 1024 * 1024
        ),
        cost_estimate=pl.CostEstimate(
            flops=flops, bytes_accessed=8 * rows * share, transcendentals=0
        ),
    )(first_factor, second_factor, result_in, pivot_scale.reshape(1, -1))


def solution(mesh):
    bands, lanes = mesh.shape["band"], mesh.shape["lane"]

    def body(first_factor, second_factor, result_in, pivot_scale):
        fits = lanes == 4 and bands == 2 * lanes
        plan = functools.partial(on_device, bands // 2) if fits else gathered
        return plan(first_factor, second_factor, result_in, pivot_scale)

    return jax.shard_map(
        body,
        mesh=mesh,
        in_specs=(P("band", "lane"), P("band", "lane"), P("band", "lane"), P()),
        out_specs=P("band", "lane"),
        check_vma=False,
    )
```

```python
import functools
import heapq

import jax
import jax.numpy as jnp
from jax import lax
from jax.experimental import pallas as pl
from jax.experimental.pallas import tpu as pltpu
from jax.sharding import PartitionSpec as P

MESH = pl.DeviceIdType.MESH
PIECES = 8
CHUNKS = 8
RELAYED = (1, 2, 3, 6, 7)
TAIL = (64, 32, 32)
FIRST, SECOND = 2, 3
X0, X1, D0, D1, H = 0, 1, 2, 3, 4
START, BLOCK, HOP = 3.3, 11.6, 2.4


def route():
    half = PIECES // 2
    rank = {X0: 0, H: 0, X1: 1, D1: 4, D0: 5}

    def urgency(item, part):
        return rank[item] + (2 * (part // half) if item not in (D0, D1) else 0)

    here, queued, busy, order, events = {}, {}, {}, {}, []

    def push(when, kind, *what):
        heapq.heappush(events, (when, len(events), kind, what))

    def send(role, way, item, part, lands, when):
        link = (role, way)
        queued.setdefault(link, []).append((urgency(item, part), part, item, lands))
        push(when, "free", link)

    for part in range(PIECES):
        for role, item in ((0, D0), (1, D1), (3, H)):
            push(START, "land", role, item, part)
        send(2, "y", X1, part, (1, X1), START)
        send(3, "y", X0, part, (0, X0), START)
    while events:
        when, _, kind, what = heapq.heappop(events)
        if kind == "free":
            (link,) = what
            if busy.get(link, 0.0) > when + 1e-9 or not queued.get(link):
                continue
            queued[link].sort()
            _, part, item, (role, becomes) = queued[link].pop(0)
            order.setdefault(link, []).append((item, part))
            busy[link] = when + BLOCK / PIECES
            push(busy[link], "free", link)
            push(busy[link] + HOP, "land", role, becomes, part)
            continue
        role, item, part = what
        here[role, item, part] = when
        if item == H:
            if role > 1 or (role == 1 and part in RELAYED):
                send(role, "d", H, part, (role - 1, H), when)
            if role < 2:
                send(role, "y", H, part, (2 if role == 1 else 3, X0), when)
        elif role == 1 and item in (X1, D1):
            send(role, "d", item, part, (0, item), when)
        if (
            (item == D0 and role < 3)
            or (item in (X1, D1) and role in (1, 2))
            or (item == X0 and (role == 0 or (role == 2 and part not in RELAYED)))
        ):
            send(role, "u", item, part, (role + 1, item), when)
    plans = [[], [], [], []]
    for (role, item, part), when in here.items():
        if (role, item) != (3, H):
            plans[role].append((max(when, START + 1.0), -1, "wait", item, part))
    for (role, way), sends in order.items():
        issued = START
        for index, (item, part) in enumerate(sends):
            if role < 2 or way != "y":
                issued = max(issued, here[role, item, part])
            plans[role].append((issued, index, way, item, part))
    return [sorted(plan) for plan in plans]


def gathered(first_factor, second_factor, result_in, pivot_scale):
    share = first_factor.shape[1]
    part_scale = lax.dynamic_slice_in_dim(pivot_scale, lax.axis_index("lane") * share, share)
    scaled_left = (first_factor.astype(jnp.float32) * part_scale).astype(jnp.bfloat16)
    left_line = lax.all_gather(scaled_left, "lane", axis=1, tiled=True)
    right = lax.all_gather(second_factor, "band", axis=0, tiled=True)
    updated = result_in - jnp.dot(left_line, right, preferred_element_type=jnp.float32)
    row_power = lax.psum(jnp.sum(updated * updated, axis=1), "lane")
    return (
        updated * lax.rsqrt(row_power / (updated.shape[1] * lax.axis_size("lane")) + 1e-06)[:, None]
    )


def kernel(
    chips, left_hbm, right_hbm, result_hbm, scale_hbm, out_hbm,
    left, right, helper, result, factors, early, outgoing, incoming, norm_out, norm_in,
    load_sem, left_send, left_recv, right_sem, helper_sem, way_sem, peer_send, peer_recv,
    part_send, part_recv, norm_send, norm_recv, out_sem,
):
    band, lane = lax.axis_index("band"), lax.axis_index("lane")
    z, core = band // 2, band % 2
    y, x = lane // 2, lane % 2
    peer = (2 * z + 1 - core, lane)
    lane_x, lane_y, lane_d = 2 * y + 1 - x, 2 * (1 - y) + x, 2 * (1 - y) + 1 - x
    role = z * (1 - y) + (chips - 1 - z) * y
    above, below = (band + 2 - 4 * y, lane), (band - 2 + 4 * y, lane)
    across = (band, lane_y)
    rows, share = left_hbm.shape
    lanes = 4
    depth, width = right_hbm.shape
    half = PIECES // 2
    piece, wide = depth // half, width // 2
    chunk = rows // CHUNKS
    own_at = pl.multiple_of((x + y) % 2 * share, share)
    other_at = pl.multiple_of((x + y + 1) % 2 * share, share)

    last = CHUNKS - 1
    sizes = (chunk,) * last + TAIL
    begins = [sum(sizes[:at]) for at in range(len(sizes) + 1)]

    def span(at):
        if isinstance(at, int):
            return pl.ds(begins[at], sizes[at])
        return pl.ds(pl.multiple_of(at * chunk, chunk), chunk)

    load_left = pltpu.make_async_copy(left_hbm, left.at[:, pl.ds(own_at, share)], load_sem.at[0])
    load_left.start()
    load_factors = pltpu.make_async_copy(scale_hbm, factors, load_sem.at[2])
    load_factors.start()
    load_result = pltpu.make_async_copy(result_hbm, result, load_sem.at[1])

    barrier = pltpu.get_barrier_semaphore()
    for other in (lane_x, lane_y):
        pl.semaphore_signal(barrier, inc=1, device_id=(band, other), device_id_type=MESH)
    pl.semaphore_signal(barrier, inc=1, device_id=peer, device_id_type=MESH)

    @pl.when(role < chips - 1)
    def _():
        pl.semaphore_signal(barrier, inc=1, device_id=above, device_id_type=MESH)

    @pl.when(role > 0)
    def _():
        pl.semaphore_signal(barrier, inc=1, device_id=below, device_id_type=MESH)

    pl.semaphore_wait(barrier, 3 + (role + chips - 1) // chips + (2 * chips - 2 - role) // chips)

    def left_copy(at):
        return pltpu.make_async_remote_copy(
            left_hbm.at[span(at), :], left.at[span(at), pl.ds(own_at, share)],
            left_send.at[0], left_recv.at[at], device_id=(band, lane_x), device_id_type=MESH,
        )

    def left_arrival(at):
        return pltpu.make_async_remote_copy(
            left_hbm.at[span(at), :], left.at[span(at), pl.ds(other_at, share)],
            left_send.at[0], left_recv.at[at], device_id=(band, lane_x), device_id_type=MESH,
        )

    def place(slot, part, of_core):
        start = (slot % 2 * 2 + of_core) * depth + part % half * piece
        return right.at[
            slot // 2 * 2 + part // half, pl.ds(pl.multiple_of(start, piece), piece), :
        ]

    def own_piece(part):
        return right_hbm.at[
            pl.ds(part % half * piece, piece), pl.ds(part // half * wide, wide)
        ]

    def send(of_role, way, item, part):
        slot = X0 if item == H else item
        at = slot * PIECES + part
        if slot == of_role + D0 or (of_role, way) == (2, "y") or of_role == 3:
            source = own_piece(part)
        else:
            source = helper.at[part] if item == H else place(slot, part, core)
        target, came = place(slot, part, core), right_sem.at[at]
        there, gone = {"u": above, "d": below, "y": across}[way], way_sem.at["udy".index(way)]
        if item == H and way == "d":
            target, came = helper.at[part], helper_sem.at[part]
        return pltpu.make_async_remote_copy(
            source, target, gone, came, device_id=there, device_id_type=MESH
        )

    def local_copy(slot, part):
        return pltpu.make_async_copy(
            own_piece(part), place(slot, part, core), right_sem.at[slot * PIECES + part]
        )

    def to_peer(slot, part, of_core):
        group = {X0: 0, X1: 0, D1: 2, D0: 3}[slot] + (slot != D1) * (part // half)
        ref = place(slot, part, of_core)
        return pltpu.make_async_remote_copy(
            ref, ref, peer_send.at[0], peer_recv.at[group], device_id=peer, device_id_type=MESH
        )

    def await_bytes(ref, semaphore):
        pltpu.make_async_copy(ref, ref, semaphore).wait()

    def await_pieces(count, semaphore):
        blocks = next(k for k in (4, 3, 2, 1) if count % k == 0)
        await_bytes(right.at[pl.ds(0, blocks), pl.ds(0, count // blocks * piece), :], semaphore)

    def arrival(item, part):
        if item == H:
            ref, came = helper.at[part], helper_sem.at[part]
        else:
            ref, came = place(item, part, core), right_sem.at[item * PIECES + part]
        return pltpu.make_async_remote_copy(
            ref, ref, came, came, device_id=peer, device_id_type=MESH
        )

    plans = route()

    reach = [
        [
            max(when for when, _, way, item, part in plan if way == "wait" and wanted(item, part))
            for wanted in (
                lambda item, part: item in (X0, X1) and part < half,
                lambda item, part: item in (X0, X1),
                lambda item, part: item == D1,
                lambda item, part: item == D0 and part < half,
                lambda item, part: item in (D0, D1),
            )
        ]
        for plan in plans
    ]
    taken = [0.0] * 4

    def take(until, needs=((),) * 4):
        for of_role in range(4):
            due = max([until] + [reach[of_role][need] for need in needs[of_role]])
            steps = [step for step in plans[of_role] if taken[of_role] < step[0] <= due]
            taken[of_role] = max(due, taken[of_role])
            if not steps:
                continue

            @pl.when(role == of_role)
            def _():
                for _, _, way, item, part in steps:
                    if way != "wait":
                        send(of_role, way, item, part).start()
                        continue
                    arrival(item, part).wait_recv()
                    if item != H:
                        to_peer(item, part, core).start()

    def await_peer(group):
        await_pieces(PIECES if group < 3 else half, peer_recv.at[group])

    def scale(at, start, of_lane):
        factor = factors[:, pl.ds(pl.multiple_of(of_lane * share, share), share)]
        window = left.at[span(at), pl.ds(start, share)]
        window[...] = (window[...].astype(jnp.float32) * factor).astype(jnp.bfloat16)

    def take_left(at):
        left_arrival(at).wait_recv()
        scale(at, other_at, lane_x)

    def part_copy(side, at):
        return pltpu.make_async_remote_copy(
            outgoing.at[side, span(at), :], incoming.at[side, span(at), :],
            part_send.at[0], part_recv.at[(at >= last) * 1 if isinstance(at, int) else 0],
            device_id=across, device_id_type=MESH,
        )

    def partial(side, rows_at, inner):
        return jnp.dot(
            left[rows_at, inner], right[side, inner, :], preferred_element_type=jnp.float32
        )

    def send_part(side, at):
        if isinstance(at, int) and at >= last:
            early_at = pl.ds(begins[at] - last * chunk, sizes[at])
            part = early[side, early_at, :] + partial(side, span(at), pl.ds(other_at, share))
        else:
            part = partial(side, span(at), pl.ds(0, 2 * share))
        outgoing[side, span(at), :] = part.astype(jnp.bfloat16)
        part_copy(side, at).start()

    def rows_of(at):
        return pl.ds(pl.multiple_of(at * chunk, chunk), chunk)

    def keep(block, at, sides=(0, 1)):
        inner = pl.ds(block * share, share)
        for side in sides:
            columns = slice(side * wide, (side + 1) * wide)
            result[rows_of(at), columns] = result[rows_of(at), columns] - jnp.dot(
                left[rows_of(at), inner], right[2 + side, inner, :],
                preferred_element_type=jnp.float32,
            )

    def finish(at):
        power = jnp.zeros((chunk, 128), jnp.float32)
        for side in range(2):
            columns = slice(side * wide, (side + 1) * wide)
            updated = result[rows_of(at), columns] - incoming[side, rows_of(at), :].astype(
                jnp.float32
            )
            result[rows_of(at), columns] = updated
            for k in range(0, wide, 128):
                power += updated[:, k : k + 128] * updated[:, k : k + 128]
        norm_out[:, rows_of(at)] = jnp.sum(power.T, axis=0, keepdims=True)

    def norms(group):
        rows_at = pl.ds(group * last * chunk, chunk if group else last * chunk)
        return [
            pltpu.make_async_remote_copy(
                norm_out.at[:, rows_at], norm_in.at[k, :, rows_at],
                norm_send.at[0], norm_recv.at[group],
                device_id=(band, other), device_id_type=MESH,
            )
            for k, other in enumerate((lane_x, lane_y, lane_d))
        ]

    def out_copy(group):
        rows_at = pl.ds(group * last * chunk, chunk if group else last * chunk)
        return pltpu.make_async_copy(
            result.at[rows_at, :], out_hbm.at[rows_at, :], out_sem.at[group]
        )

    def rescale(at):
        power = norm_out[:, rows_of(at)]
        for k in range(3):
            power = power + norm_in[k, :, rows_of(at)]
        factor = lax.rsqrt(power / (width * lanes) + 1e-06)
        factor = jnp.broadcast_to(factor, (128, chunk)).T
        for k in range(0, width, 128):
            result[rows_of(at), k : k + 128] = result[rows_of(at), k : k + 128] * factor

    scope = jax.named_scope
    for at in range(last):
        left_copy(at).start()

    @pl.when(core == 0)
    def _():
        for at in range(last, len(sizes)):
            left_copy(at).start()

    take(START)

    @pl.when(role == 0)
    def _():
        for part in range(PIECES):
            local_copy(D0, part).start()

    @pl.when(role == 1)
    def _():
        for part in range(PIECES):
            local_copy(D1, part).start()

    load_result.start()
    with scope("own"):
        load_factors.wait()
        load_left.wait()
        pl.loop(0, CHUNKS)(lambda at: scale(at, own_at, lane))

    def keep_some(block, begin, end, sides=(0, 1)):
        with scope(f"keep{block}_{end}_{sides[0]}"):
            pl.loop(begin, end)(lambda i: keep(block, i, sides))

    needed = {
        last - 2: ((2, 4), (2, 4), (2,), (2,)),
        last - 1: ((), (), (4,), (3,)),
        len(sizes) - 1: ((), (), (), (4,)),
    }
    for at in range(len(sizes)):
        due = START + 4 * BLOCK * begins[at + 1] / rows + 0.7
        with scope(f"take{at}"):
            take(due, needed.get(at, ((),) * 4))
        with scope(f"left{at}"):
            left_arrival(at).wait_recv()
        if at == last - 1:

            @pl.when(core == 1)
            def _():
                for late in range(last, len(sizes)):
                    left_copy(late).start()

        with scope(f"scale{at}"):
            scale(at, other_at, lane_x)
        for side, ready in ((0, FIRST), (1, SECOND)):
            if at == ready:
                take(0.0, ((side,),) * 4)
                with scope(f"await_x{side}"):
                    await_peer(side)
                with scope(f"parts{side}"):
                    pl.loop(0, ready + 1)(lambda i: send_part(side, i))
            elif at > ready:
                with scope(f"part{side}_{at}"):
                    send_part(side, at)
        if at == SECOND:
            with scope("early"):
                for side in range(2):
                    early[side] = partial(
                        side, pl.ds(last * chunk, chunk), pl.ds(own_at, share)
                    )
        if at == last - 2:
            with scope("await_d1"):
                await_peer(2)
                load_result.wait()
            keep_some(1, 0, last - 1)

            @pl.when(role < 2)
            def _():
                await_peer(3)
                await_peer(4)
                keep_some(0, 0, last - 1)
        if at == last - 1:
            keep(1, last - 1)

            @pl.when(role < 2)
            def _():
                keep(0, last - 1)

            @pl.when(role == 2)
            def _():
                await_peer(3)
                await_peer(4)
                keep_some(0, 0, 3)

            @pl.when(role == 3)
            def _():
                await_peer(3)
                keep_some(0, 0, last - 1, (0,))

    @pl.when(role == 2)
    def _():
        keep_some(0, 3, last)

    @pl.when(role == 3)
    def _():
        keep(0, last - 1, (0,))
        await_peer(4)
        keep_some(0, 0, last, (1,))

    with scope("await_parts"):
        await_bytes(incoming.at[:, pl.ds(0, last * chunk), :], part_recv.at[0])
    with scope("finish"):
        pl.loop(0, last, unroll=True)(finish)
        for copy in norms(0):
            copy.start()
    with scope("keep_last"):
        keep(1, last)
        keep(0, last)
    with scope("await_tail"):
        await_bytes(incoming.at[:, pl.ds(last * chunk, chunk), :], part_recv.at[1])
    with scope("finish_tail"):
        finish(last)
        for copy in norms(1):
            copy.start()
    with scope("await_norm0"):
        await_bytes(norm_in.at[:, :, pl.ds(0, last * chunk)], norm_recv.at[0])
    with scope("rescale0"):
        pl.loop(0, last, unroll=True)(rescale)
        out_copy(0).start()
    with scope("await_norm1"):
        await_bytes(norm_in.at[:, :, pl.ds(last * chunk, chunk)], norm_recv.at[1])
    with scope("rescale1"):
        rescale(last)
        out_copy(1).start()

    with scope("sends"):
        await_bytes(left_hbm, left_send.at[0])
        await_bytes(outgoing, part_send.at[0])
        await_bytes(norm_in, norm_send.at[0])
        await_pieces(4 * PIECES, peer_send.at[0])
        for of_role in range(4):
            @pl.when(role == of_role)
            def _():
                for index, way in enumerate("udy"):
                    count = sum(step[2] == way for step in plans[of_role])
                    if count:
                        await_pieces(count, way_sem.at[index])
    with scope("out"):
        for group in range(2):
            out_copy(group).wait()


def on_device(chips, first_factor, second_factor, result_in, pivot_scale):
    rows, share = first_factor.shape
    depth, width = second_factor.shape
    slots, parts = 4 * PIECES, CHUNKS - 1 + len(TAIL)
    dma = pltpu.SemaphoreType.DMA
    flops = 2 * rows * share * 4 * width
    return pl.pallas_call(
        functools.partial(kernel, chips),
        out_shape=pltpu.VMEM((rows, width), jnp.float32),
        in_specs=[
            pl.BlockSpec(memory_space=pltpu.HBM),
            pl.BlockSpec(memory_space=pltpu.HBM),
            pl.BlockSpec(memory_space=pltpu.HBM),
            pl.BlockSpec(memory_space=pltpu.HBM),
        ],
        out_specs=pl.BlockSpec(memory_space=pl.ANY),
        scratch_shapes=[
            pltpu.VMEM((rows, 2 * share), jnp.bfloat16),
            pltpu.VMEM((4, 4 * depth, width // 2), jnp.bfloat16),
            pltpu.VMEM((PIECES, 2 * depth // PIECES, width // 2), jnp.bfloat16),
            pltpu.VMEM((rows, width), jnp.float32),
            pltpu.VMEM((1, 4 * share), jnp.float32),
            pltpu.VMEM((2, rows // CHUNKS, width // 2), jnp.float32),
            pltpu.VMEM((2, rows, width // 2), jnp.bfloat16),
            pltpu.VMEM((2, rows, width // 2), jnp.bfloat16),
            pltpu.VMEM((1, rows), jnp.float32),
            pltpu.VMEM((3, 1, rows), jnp.float32),
            dma((3,)),
            dma((1,)),
            dma((parts,)),
            dma((slots,)),
            dma((PIECES,)),
            dma((3,)),
            dma((1,)),
            dma((5,)),
            dma((1,)),
            dma((2,)),
            dma((1,)),
            dma((2,)),
            dma((2,)),
        ],
        compiler_params=pltpu.CompilerParams(
            collective_id=0, has_side_effects=True, vmem_limit_bytes=56 * 1024 * 1024
        ),
        cost_estimate=pl.CostEstimate(
            flops=flops, bytes_accessed=8 * rows * share, transcendentals=0
        ),
    )(first_factor, second_factor, result_in, pivot_scale.reshape(1, -1))


def solution(mesh):
    bands, lanes = mesh.shape["band"], mesh.shape["lane"]

    def body(first_factor, second_factor, result_in, pivot_scale):
        fits = lanes == 4 and bands == 2 * lanes
        plan = functools.partial(on_device, bands // 2) if fits else gathered
        return plan(first_factor, second_factor, result_in, pivot_scale)

    return jax.shard_map(
        body,
        mesh=mesh,
        in_specs=(P("band", "lane"), P("band", "lane"), P("band", "lane"), P()),
        out_specs=P("band", "lane"),
        check_vma=False,
    )
```
